32 devices in a mesh: dp: 2 (over z, core), tp: 16 (over x, y).
Axes of the slice: x: 4, y: 4, z: 1, core: 2. Of those that a mesh axis runs over, the one named last changes fastest.
The devices are a block of a 4x4x8 slice.
Arguments:
- x: bfloat16 [3072, 12288], P(('dp', 'tp')), parts along dimension 0
- w_gate: bfloat16 [12288, 28672], P(None, 'tp')
- w_up: bfloat16 [12288, 28672], P(None, 'tp')
- w_down: bfloat16 [28672, 12288], P('tp')
Outputs:
- output: bfloat16 [3072, 12288], P(('dp', 'tp')), parts along dimension 0
There are 2 independent parts. The reference program is written for one: setup_inputs(seed, part) draws one part's arguments, and reference() takes and returns one part's arrays. A program takes and returns all parts, laid end to end along the dimension named above; an argument that names none is the same for every part.
All inputs are finite; a program needn't handle non-finite values.
Results may differ from the reference program's by a relative error of at most 0.016.
Values are sent between devices in bfloat16 or wider.
A program may use at most 768 MiB of HBM per device.

```python
import jax
import jax.numpy as jnp

ROWS = 1536
D = 12288
FF = 28672


def setup_inputs(seed: int = 0, part: int = 0) -> dict:
    kx, kg, ku, kd = jax.random.split(jax.random.key(seed), 4)
    drawn = {
        "x": jax.random.normal(jax.random.fold_in(kx, part), (ROWS, D), jnp.float32),
        "w_gate": jax.random.normal(kg, (D, FF), jnp.float32) * D**-0.5,
        "w_up": jax.random.normal(ku, (D, FF), jnp.float32) * D**-0.5,
        "w_down": jax.random.normal(kd, (FF, D), jnp.float32) * FF**-0.5,
    }
    return {k: v.astype(jnp.bfloat16) for k, v in drawn.items()}


def reference(x, w_gate, w_up, w_down):
    gate = jnp.dot(x, w_gate, preferred_element_type=jnp.float32)
    up = jnp.dot(x, w_up, preferred_element_type=jnp.float32)
    hidden = (jax.nn.silu(gate) * up).astype(jnp.bfloat16)
    return jnp.dot(hidden, w_down, preferred_element_type=jnp.float32).astype(jnp.bfloat16)
```

```python
import functools
import math

import jax
import jax.numpy as jnp
from jax import lax
from jax.experimental import pallas as pl
from jax.experimental.pallas import tpu as pltpu
from jax.sharding import PartitionSpec as P

COMPUTE = True
COMM = True

BF16, F32 = jnp.bfloat16, jnp.float32
RINGS = 4
ROWS = 8
BLOCKS = 4
K_TILES = 24
N_TILES = 12
WEIGHT_SLOTS = 3
HOP_SLOTS = 4


def kernel(
    n, x_ref, wg_ref, wu_ref, wd_ref, y_ref, xg_ref, t_ref,
    wg_buf, wu_buf, wd_buf, x_buf, acc_g, acc_u, hid, t_buf, term_buf, send_buf, sum_buf,
    wgu_sem, wd_sem, x_sem, t_sem, term_sem, y_sem,
    ag_send, ag_recv, rs_send, rs_recv, credit,
):
    m, d = x_ref.shape
    part = m // RINGS
    subs = part // ROWS
    per_hop = RINGS * subs
    block = n * m // BLOCKS
    kt, nt = d // K_TILES, d // N_TILES
    side = math.isqrt(n)

    me = lax.axis_index("tp")
    px, py = me // side, me % side
    diagonal = (px + py) % side

    def by_x(t):
        a, b = t // side, t % side
        return a * side + (b - a + side) % side

    def by_y(t):
        a, b = t // side, t % side
        return (b - a + side) % side * side + a

    at_x, at_y = px * side + diagonal, py * side + diagonal
    ahead_x, behind_x = by_x((at_x + 1) % n), by_x((at_x + n - 1) % n)
    ahead_y, behind_y = by_y((at_y + 1) % n), by_y((at_y + n - 1) % n)
    target = (ahead_x, behind_x, ahead_y, behind_y)
    origin = (behind_x, ahead_x, behind_y, ahead_y)

    def rows_of(s, r, j):
        return pl.ds(pl.multiple_of(((s * RINGS + r) * subs + j) * ROWS, ROWS), ROWS)

    def ag_copy(s, r, j, src):
        return pltpu.make_async_remote_copy(
            src_ref=src,
            dst_ref=xg_ref.at[rows_of(s + 1, r, j), :],
            send_sem=ag_send.at[r * subs + j],
            recv_sem=ag_recv.at[s * per_hop + r * subs + j],
            device_id={"tp": target[r]},
            device_id_type=pl.DeviceIdType.MESH,
        )

    def ag_first():
        for j in range(subs):
            for r in range(RINGS):
                ag_copy(0, r, j, x_ref.at[rows_of(0, r, j), :]).start()

    def ag_service(q):
        s, j = q // subs + 1, q % subs
        for r in range(RINGS):
            ag_copy(s - 1, r, j, xg_ref.at[rows_of(s, r, j), :]).wait_recv()

            @pl.when(s < n - 1)
            def _():
                copy = ag_copy(s, r, j, xg_ref.at[rows_of(s, r, j), :])
                copy.wait_send()
                copy.start()

    def ag_last():
        for j in range(subs):
            for r in range(RINGS):
                ag_copy(0, r, j, x_ref.at[rows_of(0, r, j), :]).wait_send()

    def term_copy(p, r):
        h, j = p // subs + 1, p % subs
        return pltpu.make_async_copy(
            t_ref.at[rows_of(h % n, r, j), :], term_buf.at[p % 2, r], term_sem.at[p % 2, r]
        )

    def term_start(p):
        for r in range(RINGS):
            term_copy(p, r).start()

    def rs_copy(h, r, j):
        return pltpu.make_async_remote_copy(
            src_ref=send_buf.at[r * subs + j],
            dst_ref=sum_buf.at[(h + 1) % HOP_SLOTS * per_hop + r * subs + j],
            send_sem=rs_send.at[r * subs + j],
            recv_sem=rs_recv.at[(h + 1) % HOP_SLOTS * per_hop + r * subs + j],
            device_id={"tp": target[r]},
            device_id_type=pl.DeviceIdType.MESH,
        )

    def rs_add(p, r, first):
        h, j = p // subs + 1, p % subs
        term_copy(p, r).wait()
        total = term_buf[p % 2, r]
        if not first:
            rs_copy(h - 1, r, j).wait_recv()
            rs_copy(h - 1, r, j).wait_send()
            total += sum_buf[h % HOP_SLOTS * per_hop + r * subs + j].astype(F32)
        send_buf[r * subs + j] = total.astype(BF16)
        if not first:

            @pl.when(h + HOP_SLOTS <= n)
            def _():
                pl.semaphore_signal(
                    credit.at[r * subs + j],
                    inc=1,
                    device_id={"tp": origin[r]},
                    device_id_type=pl.DeviceIdType.MESH,
                )

    def rs_service(p, first):
        h, j = p // subs + 1, p % subs
        for r in range(RINGS):
            rs_add(p, r, first)
        for r in range(RINGS):
            if not first:

                @pl.when(h > HOP_SLOTS)
                def _():
                    pl.semaphore_wait(credit.at[r * subs + j], 1)

            rs_copy(h, r, j).start()
        term_start(p + 1)

    def y_copy(r, j):
        return pltpu.make_async_copy(
            send_buf.at[r * subs + j], y_ref.at[rows_of(0, r, j), :], y_sem.at[r * subs + j]
        )

    def gu_copies(g):
        k = pl.ds(pl.multiple_of(g % K_TILES * kt, kt), kt)
        slot = g % WEIGHT_SLOTS
        return (
            pltpu.make_async_copy(wg_ref.at[k, :], wg_buf.at[slot], wgu_sem.at[slot, 0]),
            pltpu.make_async_copy(wu_ref.at[k, :], wu_buf.at[slot], wgu_sem.at[slot, 1]),
        )

    def wd_copy(e):
        cols = pl.ds(pl.multiple_of(e % N_TILES * nt, nt), nt)
        slot = e % WEIGHT_SLOTS
        return pltpu.make_async_copy(wd_ref.at[:, cols], wd_buf.at[slot], wd_sem.at[slot])

    def x_start(b, i):
        k = pl.ds(pl.multiple_of(i * kt, kt), kt)

        @pl.when(b == 0)
        def _():
            pltpu.make_async_copy(
                x_ref.at[:, k], x_buf.at[i % 2, pl.ds(0, m), :], x_sem.at[i % 2]
            ).start()
            pltpu.make_async_copy(
                xg_ref.at[pl.ds(m, block - m), k], x_buf.at[i % 2, pl.ds(m, block - m), :], x_sem.at[i % 2]
            ).start()

        @pl.when(b > 0)
        def _():
            x_copy(b, i).start()

    def x_copy(b, i):
        k = pl.ds(pl.multiple_of(i * kt, kt), kt)
        return pltpu.make_async_copy(
            xg_ref.at[pl.ds(pl.multiple_of(b * block, block), block), k], x_buf.at[i % 2], x_sem.at[i % 2]
        )

    def t_copy(b, i):
        rows = pl.ds(pl.multiple_of(b * block, block), block)
        cols = pl.ds(pl.multiple_of(i * nt, nt), nt)
        return pltpu.make_async_copy(t_buf.at[i % 2], t_ref.at[rows, cols], t_sem.at[i % 2])

    def t_drain(b):
        t_copy(b, N_TILES - 2).wait()
        t_copy(b, N_TILES - 1).wait()

    f = wg_ref.shape[1]
    step_n = 256

    def gate_up(b, i):
        g = b * K_TILES + i
        slot = g % WEIGHT_SLOTS

        @pl.when(i == 0)
        def _():
            @pl.when(b > 0)
            def _():
                t_drain(b - 1)

            acc_g[...] = jnp.zeros_like(acc_g)
            acc_u[...] = jnp.zeros_like(acc_u)

        for copy in gu_copies(g):
            copy.wait()

        @pl.when(g + WEIGHT_SLOTS - 1 < BLOCKS * K_TILES)
        def _():
            for copy in gu_copies(g + WEIGHT_SLOTS - 1):
                copy.start()

        x_copy(b, i).wait()

        @pl.when(i + 1 < K_TILES)
        def _():
            x_start(b, i + 1)

        if COMPUTE:
            xt = x_buf[i % 2]
            for c in range(0, f, step_n):
                acc_g[:, c : c + step_n] += jnp.dot(xt, wg_buf[slot, :, c : c + step_n], preferred_element_type=F32)
                acc_u[:, c : c + step_n] += jnp.dot(xt, wu_buf[slot, :, c : c + step_n], preferred_element_type=F32)

        @pl.when(i == K_TILES - 1)
        def _():
            def chunk(c, _):
                rows = pl.ds(pl.multiple_of(c * 16, 16), 16)
                hid[rows, :] = (jax.nn.silu(acc_g[rows, :]) * acc_u[rows, :]).astype(BF16)
                return 0

            lax.fori_loop(0, block // 16, chunk, 0)

    def down(b, i):
        e = b * N_TILES + i
        slot = e % WEIGHT_SLOTS
        wd_copy(e).wait()

        @pl.when(e + WEIGHT_SLOTS - 1 < BLOCKS * N_TILES)
        def _():
            wd_copy(e + WEIGHT_SLOTS - 1).start()

        @pl.when(i >= 2)
        def _():
            t_copy(b, i - 2).wait()

        if COMPUTE:
            for c in range(0, nt, step_n):
                t_buf[i % 2, :, c : c + step_n] = jnp.dot(
                    hid[...], wd_buf[slot, :, c : c + step_n], preferred_element_type=F32
                )
        t_copy(b, i).start()

        @pl.when((i == N_TILES - 1) & (b < BLOCKS - 1))
        def _():
            x_start(b + 1, 0)

    barrier = pltpu.get_barrier_semaphore()
    for r in range(RINGS):
        pl.semaphore_signal(barrier, inc=1, device_id={"tp": target[r]}, device_id_type=pl.DeviceIdType.MESH)
    pl.semaphore_wait(barrier, RINGS)

    if COMM:
        ag_first()
    for e in range(WEIGHT_SLOTS - 1):
        for copy in gu_copies(e):
            copy.start()
        wd_copy(e).start()

    ticks = K_TILES + N_TILES
    lead = (n // BLOCKS - 1) * subs
    ag_pieces = (n - 1) * subs
    ag_num, ag_den = 2, 5
    rs_at = -((lead - ag_pieces) * ag_den // ag_num) + 2
    rs_num, rs_den = 4, 7

    if COMM:
        lax.fori_loop(0, lead, lambda q, _: (ag_service(q), 0)[1], 0)
    x_start(0, 0)

    def tick(t, _):
        b, i = t // ticks, t % ticks

        @pl.when(i < K_TILES)
        def _():
            gate_up(b, i)

        @pl.when(i >= K_TILES)
        def _():
            down(b, i - K_TILES)

        if COMM:
            q = lead + t * ag_num // ag_den

            @pl.when((q < ag_pieces) & (t * ag_num % ag_den < ag_num))
            def _():
                ag_service(q)

            @pl.when(t == rs_at - 1)
            def _():
                term_start(0)

            u = t - rs_at
            p = u * rs_num // rs_den

            @pl.when((u >= 0) & (u * rs_num % rs_den < rs_num))
            def _():
                @pl.when(p < subs)
                def _():
                    rs_service(p, True)

                @pl.when(p >= subs)
                def _():
                    rs_service(p, False)

        return 0

    total = BLOCKS * ticks
    lax.fori_loop(0, total, tick, 0)
    t_drain(BLOCKS - 1)
    if COMM:
        ag_last()
        p0 = ((total - 1 - rs_at) * rs_num) // rs_den + 1
        lax.fori_loop(p0, (n - 1) * subs, lambda p, _: (rs_service(p, False), 0)[1], 0)
        for j in range(subs):
            p = (n - 1) * subs + j
            for r in range(RINGS):
                rs_add(p, r, False)
                y_copy(r, j).start()
            if j + 1 < subs:
                term_start(p + 1)
        for j in range(subs):
            for r in range(RINGS):
                y_copy(r, j).wait()


def solution(mesh):
    n = mesh.shape["tp"]

    def step(x, w_gate, w_up, w_down):
        m, d = x.shape
        f = w_gate.shape[1]
        block = n * m // BLOCKS
        kt, nt = d // K_TILES, d // N_TILES
        subs = m // RINGS // ROWS
        per_hop = RINGS * subs
        dma = pltpu.SemaphoreType.DMA
        hbm = pl.BlockSpec(memory_space=pl.ANY)
        y, _, _ = pl.pallas_call(
            functools.partial(kernel, n),
            out_shape=(
                jax.ShapeDtypeStruct((m, d), BF16),
                jax.ShapeDtypeStruct((n * m, d), BF16),
                jax.ShapeDtypeStruct((n * m, d), F32),
            ),
            in_specs=[hbm] * 4,
            out_specs=(hbm,) * 3,
            scratch_shapes=[
                pltpu.VMEM((WEIGHT_SLOTS, kt, f), BF16),
                pltpu.VMEM((WEIGHT_SLOTS, kt, f), BF16),
                pltpu.VMEM((WEIGHT_SLOTS, f, nt), BF16),
                pltpu.VMEM((2, block, kt), BF16),
                pltpu.VMEM((block, f), F32),
                pltpu.VMEM((block, f), F32),
                pltpu.VMEM((block, f), BF16),
                pltpu.VMEM((2, block, nt), F32),
                pltpu.VMEM((2, RINGS, ROWS, d), F32),
                pltpu.VMEM((per_hop, ROWS, d), BF16),
                pltpu.VMEM((HOP_SLOTS * per_hop, ROWS, d), BF16),
                dma((WEIGHT_SLOTS, 2)),
                dma((WEIGHT_SLOTS,)),
                dma((2,)),
                dma((2,)),
                dma((2, RINGS)),
                dma((per_hop,)),
                dma((per_hop,)),
                dma(((n - 1) * per_hop,)),
                dma((per_hop,)),
                dma((HOP_SLOTS * per_hop,)),
                pltpu.SemaphoreType.REGULAR((per_hop,)),
            ],
            compiler_params=pltpu.CompilerParams(
                collective_id=0, has_side_effects=True, vmem_limit_bytes=64 * 1000 * 1000
            ),
        )(x, w_gate, w_up, w_down)
        return y

    return jax.shard_map(
        step,
        mesh=mesh,
        in_specs=(P(("dp", "tp"), None), P(None, "tp"), P(None, "tp"), P("tp", None)),
        out_specs=P(("dp", "tp"), None),
        check_vma=False,
    )
```

```python
import functools
import math

import jax
import jax.numpy as jnp
from jax import lax
from jax.experimental import pallas as pl
from jax.experimental.pallas import tpu as pltpu
from jax.sharding import PartitionSpec as P

COMPUTE = True
COMM = True

BF16, F32 = jnp.bfloat16, jnp.float32
RINGS = 4
ROWS = 8
BLOCKS = 4
K_TILES = 24
N_TILES = 12
WEIGHT_SLOTS = 3
X_SLOTS = 3
GATHER_TICKS = 77
HOP_SLOTS = 4


def kernel(
    n, x_ref, wg_ref, wu_ref, wd_ref, y_ref, xg_ref, t_ref,
    wg_buf, wu_buf, wd_buf, x_buf, acc_g, acc_u, hid, t_buf, term_buf, send_buf, sum_buf,
    wgu_sem, wd_sem, x_sem, t_sem, term_sem, y_sem,
    ag_send, ag_recv, rs_send, rs_recv, credit,
):
    m, d = x_ref.shape
    part = m // RINGS
    subs = part // ROWS
    per_hop = RINGS * subs
    block = n * m // BLOCKS
    kt, nt = d // K_TILES, d // N_TILES
    side = math.isqrt(n)

    me = lax.axis_index("tp")
    px, py = me // side, me % side
    diagonal = (px + py) % side

    def by_x(t):
        a, b = t // side, t % side
        return a * side + (b - a + side) % side

    def by_y(t):
        a, b = t // side, t % side
        return (b - a + side) % side * side + a

    at_x, at_y = px * side + diagonal, py * side + diagonal
    ahead_x, behind_x = by_x((at_x + 1) % n), by_x((at_x + n - 1) % n)
    ahead_y, behind_y = by_y((at_y + 1) % n), by_y((at_y + n - 1) % n)
    target = (ahead_x, behind_x, ahead_y, behind_y)
    origin = (behind_x, ahead_x, behind_y, ahead_y)

    def rows_of(s, r, j):
        return pl.ds(pl.multiple_of(((s * RINGS + r) * subs + j) * ROWS, ROWS), ROWS)

    def ag_copy(s, r, j, src):
        return pltpu.make_async_remote_copy(
            src_ref=src,
            dst_ref=xg_ref.at[rows_of(s + 1, r, j), :],
            send_sem=ag_send.at[r * subs + j],
            recv_sem=ag_recv.at[s * per_hop + r * subs + j],
            device_id={"tp": target[r]},
            device_id_type=pl.DeviceIdType.MESH,
        )

    def ag_first():
        for j in range(subs):
            for r in range(RINGS):
                ag_copy(0, r, j, x_ref.at[rows_of(0, r, j), :]).start()

    def ag_service(q):
        s, j = q // subs + 1, q % subs
        for r in range(RINGS):
            copy = ag_copy(s, r, j, xg_ref.at[rows_of(s, r, j), :])
            ag_copy(s - 1, r, j, xg_ref.at[rows_of(s, r, j), :]).wait_recv()
            copy.wait_send()
            copy.start()

    def ag_last(j):
        for r in range(RINGS):
            copy = ag_copy(n - 2, r, j, xg_ref.at[rows_of(n - 2, r, j), :])
            copy.wait_send()
            copy.wait_recv()

    def term_copy(p, r):
        h, j = p // subs + 1, p % subs
        return pltpu.make_async_copy(
            t_ref.at[rows_of(h % n, r, j), :], term_buf.at[p % 2, r], term_sem.at[p % 2, r]
        )

    def term_start(p):
        for r in range(RINGS):
            term_copy(p, r).start()

    def rs_copy(h, r, j):
        return pltpu.make_async_remote_copy(
            src_ref=send_buf.at[r * subs + j],
            dst_ref=sum_buf.at[(h + 1) % HOP_SLOTS * per_hop + r * subs + j],
            send_sem=rs_send.at[r * subs + j],
            recv_sem=rs_recv.at[(h + 1) % HOP_SLOTS * per_hop + r * subs + j],
            device_id={"tp": target[r]},
            device_id_type=pl.DeviceIdType.MESH,
        )

    def rs_add(p, r, first):
        h, j = p // subs + 1, p % subs
        term_copy(p, r).wait()
        total = term_buf[p % 2, r]
        if not first:
            rs_copy(h - 1, r, j).wait_recv()
            rs_copy(h - 1, r, j).wait_send()
            total += sum_buf[h % HOP_SLOTS * per_hop + r * subs + j].astype(F32)
        send_buf[r * subs + j] = total.astype(BF16)
        if not first:

            @pl.when(h + HOP_SLOTS <= n)
            def _():
                pl.semaphore_signal(
                    credit.at[r * subs + j],
                    inc=1,
                    device_id={"tp": origin[r]},
                    device_id_type=pl.DeviceIdType.MESH,
                )

    def rs_service(p, first):
        h, j = p // subs + 1, p % subs
        for r in range(RINGS):
            rs_add(p, r, first)
        for r in range(RINGS):
            if not first:

                @pl.when(h > HOP_SLOTS)
                def _():
                    pl.semaphore_wait(credit.at[r * subs + j], 1)

            rs_copy(h, r, j).start()
        term_start(p + 1)

    def y_copy(r, j):
        return pltpu.make_async_copy(
            send_buf.at[r * subs + j], y_ref.at[rows_of(0, r, j), :], y_sem.at[r * subs + j]
        )

    def gu_copies(g):
        k = pl.ds(pl.multiple_of(g % K_TILES * kt, kt), kt)
        slot = g % WEIGHT_SLOTS
        return (
            pltpu.make_async_copy(wg_ref.at[k, :], wg_buf.at[slot], wgu_sem.at[slot, 0]),
            pltpu.make_async_copy(wu_ref.at[k, :], wu_buf.at[slot], wgu_sem.at[slot, 1]),
        )

    def wd_copy(e):
        cols = pl.ds(pl.multiple_of(e % N_TILES * nt, nt), nt)
        slot = e % WEIGHT_SLOTS
        return pltpu.make_async_copy(wd_ref.at[:, cols], wd_buf.at[slot], wd_sem.at[slot])

    def x_start(b, i):
        k = pl.ds(pl.multiple_of(i * kt, kt), kt)

        @pl.when(b == 0)
        def _():
            pltpu.make_async_copy(
                x_ref.at[:, k], x_buf.at[i % X_SLOTS, pl.ds(0, m), :], x_sem.at[i % X_SLOTS]
            ).start()
            pltpu.make_async_copy(
                xg_ref.at[pl.ds(m, block - m), k], x_buf.at[i % X_SLOTS, pl.ds(m, block - m), :], x_sem.at[i % X_SLOTS]
            ).start()

        @pl.when(b > 0)
        def _():
            x_copy(b, i).start()

    def x_copy(b, i):
        k = pl.ds(pl.multiple_of(i * kt, kt), kt)
        return pltpu.make_async_copy(
            xg_ref.at[pl.ds(pl.multiple_of(b * block, block), block), k], x_buf.at[i % X_SLOTS], x_sem.at[i % X_SLOTS]
        )

    def t_copy(b, i):
        rows = pl.ds(pl.multiple_of(b * block, block), block)
        cols = pl.ds(pl.multiple_of(i * nt, nt), nt)
        return pltpu.make_async_copy(t_buf.at[i % 2], t_ref.at[rows, cols], t_sem.at[i % 2])

    def t_drain(b):
        t_copy(b, N_TILES - 2).wait()
        t_copy(b, N_TILES - 1).wait()

    f = wg_ref.shape[1]
    step_n = 256

    def gate_up(b, i):
        g = b * K_TILES + i
        slot = g % WEIGHT_SLOTS

        @pl.when(i == 0)
        def _():
            @pl.when(b > 0)
            def _():
                t_drain(b - 1)

            acc_g[...] = jnp.zeros_like(acc_g)
            acc_u[...] = jnp.zeros_like(acc_u)

        @pl.when(i + X_SLOTS - 1 < K_TILES)
        def _():
            x_start(b, i + X_SLOTS - 1)

        @pl.when(g + WEIGHT_SLOTS - 1 < BLOCKS * K_TILES)
        def _():
            for copy in gu_copies(g + WEIGHT_SLOTS - 1):
                copy.start()

        x_copy(b, i).wait()
        for copy in gu_copies(g):
            copy.wait()

        if COMPUTE:
            xt = x_buf[i % X_SLOTS]
            for c in range(0, f, step_n):
                acc_g[:, c : c + step_n] += jnp.dot(xt, wg_buf[slot, :, c : c + step_n], preferred_element_type=F32)
                acc_u[:, c : c + step_n] += jnp.dot(xt, wu_buf[slot, :, c : c + step_n], preferred_element_type=F32)

        @pl.when(i == K_TILES - 1)
        def _():
            def chunk(c, _):
                rows = pl.ds(pl.multiple_of(c * 16, 16), 16)
                hid[rows, :] = (jax.nn.silu(acc_g[rows, :]) * acc_u[rows, :]).astype(BF16)
                return 0

            lax.fori_loop(0, block // 16, chunk, 0)

    def down(b, i):
        e = b * N_TILES + i
        slot = e % WEIGHT_SLOTS
        wd_copy(e).wait()

        @pl.when(e + WEIGHT_SLOTS - 1 < BLOCKS * N_TILES)
        def _():
            wd_copy(e + WEIGHT_SLOTS - 1).start()

        @pl.when(i >= 2)
        def _():
            t_copy(b, i - 2).wait()

        if COMPUTE:
            for c in range(0, nt, step_n):
                t_buf[i % 2, :, c : c + step_n] = jnp.dot(
                    hid[...], wd_buf[slot, :, c : c + step_n], preferred_element_type=F32
                )
        t_copy(b, i).start()

        ahead = i - (N_TILES - X_SLOTS + 1)

        @pl.when((ahead >= 0) & (b < BLOCKS - 1))
        def _():
            x_start(b + 1, ahead)

    barrier = pltpu.get_barrier_semaphore()
    for r in range(RINGS):
        pl.semaphore_signal(barrier, inc=1, device_id={"tp": target[r]}, device_id_type=pl.DeviceIdType.MESH)
    pl.semaphore_wait(barrier, RINGS)

    if COMM:
        ag_first()
    for e in range(WEIGHT_SLOTS - 1):
        for copy in gu_copies(e):
            copy.start()
        wd_copy(e).start()

    ticks = K_TILES + N_TILES
    total = BLOCKS * ticks
    lead = (n // BLOCKS - 1) * subs
    forwards = (n - 2) * subs
    last_terms = (n - n // BLOCKS - 1) * subs

    def serve(z):
        @pl.when(z < forwards)
        def _():
            ag_service(z)

        @pl.when(z == forwards - 1)
        def _():
            term_start(0)

        @pl.when((z >= forwards) & (z < forwards + subs))
        def _():
            rs_service(z - forwards, True)

        @pl.when(z >= forwards + subs)
        def _():
            rs_service(z - forwards, False)

        @pl.when((z >= forwards + subs) & (z < forwards + 2 * subs))
        def _():
            ag_last(z - forwards - subs)

    if COMM:
        lax.fori_loop(0, lead, lambda q, _: (ag_service(q), 0)[1], 0)
    for i in range(X_SLOTS - 1):
        x_start(0, i)

    def tick(t, _):
        b, i = t // ticks, t % ticks

        @pl.when(i < K_TILES)
        def _():
            gate_up(b, i)

        @pl.when(i >= K_TILES)
        def _():
            down(b, i - K_TILES)

        if COMM:
            u = t * (forwards - lead)

            @pl.when((t < GATHER_TICKS) & (u % GATHER_TICKS < forwards - lead))
            def _():
                serve(lead + u // GATHER_TICKS)

            v = (t - GATHER_TICKS) * (last_terms - 1)
            rest = total - GATHER_TICKS

            @pl.when((t >= GATHER_TICKS) & (v % rest < last_terms - 1))
            def _():
                serve(forwards + v // rest)

        return 0

    lax.fori_loop(0, total, tick, 0)
    t_drain(BLOCKS - 1)
    if COMM:
        lax.fori_loop(last_terms - 1, (n - 1) * subs, lambda p, _: (rs_service(p, False), 0)[1], 0)
        for j in range(subs):
            p = (n - 1) * subs + j
            for r in range(RINGS):
                rs_add(p, r, False)
                y_copy(r, j).start()
            if j + 1 < subs:
                term_start(p + 1)
        for j in range(subs):
            for r in range(RINGS):
                y_copy(r, j).wait()


def solution(mesh):
    n = mesh.shape["tp"]

    def step(x, w_gate, w_up, w_down):
        m, d = x.shape
        f = w_gate.shape[1]
        block = n * m // BLOCKS
        kt, nt = d // K_TILES, d // N_TILES
        subs = m // RINGS // ROWS
        per_hop = RINGS * subs
        dma = pltpu.SemaphoreType.DMA
        hbm = pl.BlockSpec(memory_space=pl.ANY)
        y, _, _ = pl.pallas_call(
            functools.partial(kernel, n),
            out_shape=(
                jax.ShapeDtypeStruct((m, d), BF16),
                jax.ShapeDtypeStruct((n * m, d), BF16),
                jax.ShapeDtypeStruct((n * m, d), F32),
            ),
            in_specs=[hbm] * 4,
            out_specs=(hbm,) * 3,
            scratch_shapes=[
                pltpu.VMEM((WEIGHT_SLOTS, kt, f), BF16),
                pltpu.VMEM((WEIGHT_SLOTS, kt, f), BF16),
                pltpu.VMEM((WEIGHT_SLOTS, f, nt), BF16),
                pltpu.VMEM((X_SLOTS, block, kt), BF16),
                pltpu.VMEM((block, f), F32),
                pltpu.VMEM((block, f), F32),
                pltpu.VMEM((block, f), BF16),
                pltpu.VMEM((2, block, nt), F32),
                pltpu.VMEM((2, RINGS, ROWS, d), F32),
                pltpu.VMEM((per_hop, ROWS, d), BF16),
                pltpu.VMEM((HOP_SLOTS * per_hop, ROWS, d), BF16),
                dma((WEIGHT_SLOTS, 2)),
                dma((WEIGHT_SLOTS,)),
                dma((X_SLOTS,)),
                dma((2,)),
                dma((2, RINGS)),
                dma((per_hop,)),
                dma((per_hop,)),
                dma(((n - 1) * per_hop,)),
                dma((per_hop,)),
                dma((HOP_SLOTS * per_hop,)),
                pltpu.SemaphoreType.REGULAR((per_hop,)),
            ],
            compiler_params=pltpu.CompilerParams(
                collective_id=0, has_side_effects=True, vmem_limit_bytes=64 * 1000 * 1000
            ),
        )(x, w_gate, w_up, w_down)
        return y

    return jax.shard_map(
        step,
        mesh=mesh,
        in_specs=(P(("dp", "tp"), None), P(None, "tp"), P(None, "tp"), P("tp", None)),
        out_specs=P(("dp", "tp"), None),
        check_vma=False,
    )
```

```python
import functools
import math

import jax
import jax.numpy as jnp
from jax import lax
from jax.experimental import pallas as pl
from jax.experimental.pallas import tpu as pltpu
from jax.sharding import PartitionSpec as P

COMPUTE = True
COMM = True

BF16, F32 = jnp.bfloat16, jnp.float32
RINGS = 4
ROWS = 8
BLOCKS = 4
K_TILES = 24
N_TILES = 12
WEIGHT_SLOTS = 3
X_SLOTS = 3
GATHER_TICKS = 77
HOP_SLOTS = 3


def kernel(
    n, x_ref, wg_ref, wu_ref, wd_ref, sum_ref, own_ref, xg_ref, t_ref,
    wg_buf, wu_buf, wd_buf, x_buf, acc_g, acc_u, hid, t_buf, term_buf, send_buf, sum_buf,
    wgu_sem, wd_sem, x_sem, t_sem, term_sem, own_sem,
    ag_send, ag_recv, rs_send, rs_recv, last_recv, credit,
):
    m, d = x_ref.shape
    part = m // RINGS
    subs = part // ROWS
    per_hop = RINGS * subs
    block = n * m // BLOCKS
    kt, nt = d // K_TILES, d // N_TILES
    side = math.isqrt(n)

    me = lax.axis_index("tp")
    px, py = me // side, me % side
    diagonal = (px + py) % side

    def by_x(t):
        a, b = t // side, t % side
        return a * side + (b - a + side) % side

    def by_y(t):
        a, b = t // side, t % side
        return (b - a + side) % side * side + a

    at_x, at_y = px * side + diagonal, py * side + diagonal
    ahead_x, behind_x = by_x((at_x + 1) % n), by_x((at_x + n - 1) % n)
    ahead_y, behind_y = by_y((at_y + 1) % n), by_y((at_y + n - 1) % n)
    target = (ahead_x, behind_x, ahead_y, behind_y)
    origin = (behind_x, ahead_x, behind_y, ahead_y)

    def rows_of(s, r, j):
        return pl.ds(pl.multiple_of(((s * RINGS + r) * subs + j) * ROWS, ROWS), ROWS)

    def ag_copy(s, r, j, src):
        return pltpu.make_async_remote_copy(
            src_ref=src,
            dst_ref=xg_ref.at[rows_of(s + 1, r, j), :],
            send_sem=ag_send.at[r * subs + j],
            recv_sem=ag_recv.at[s * per_hop + r * subs + j],
            device_id={"tp": target[r]},
            device_id_type=pl.DeviceIdType.MESH,
        )

    def ag_first():
        for j in range(subs):
            for r in range(RINGS):
                ag_copy(0, r, j, x_ref.at[rows_of(0, r, j), :]).start()

    def ag_service(q):
        s, j = q // subs + 1, q % subs
        for r in range(RINGS):
            copy = ag_copy(s, r, j, xg_ref.at[rows_of(s, r, j), :])
            ag_copy(s - 1, r, j, xg_ref.at[rows_of(s, r, j), :]).wait_recv()
            copy.wait_send()
            copy.start()

    def ag_last(j):
        for r in range(RINGS):
            copy = ag_copy(n - 2, r, j, xg_ref.at[rows_of(n - 2, r, j), :])
            copy.wait_send()
            copy.wait_recv()

    def term_copy(p, r):
        h, j = p // subs + 1, p % subs
        return pltpu.make_async_copy(
            t_ref.at[rows_of(h % n, r, j), :], term_buf.at[p % 2, r], term_sem.at[p % 2, r]
        )

    def term_start(p):
        for r in range(RINGS):
            term_copy(p, r).start()

    def rs_copy(h, r, j):
        return pltpu.make_async_remote_copy(
            src_ref=send_buf.at[r * subs + j],
            dst_ref=sum_buf.at[(h + 1) % HOP_SLOTS * per_hop + r * subs + j],
            send_sem=rs_send.at[r * subs + j],
            recv_sem=rs_recv.at[(h + 1) % HOP_SLOTS * per_hop + r * subs + j],
            device_id={"tp": target[r]},
            device_id_type=pl.DeviceIdType.MESH,
        )

    def own_copy():
        return pltpu.make_async_copy(t_ref.at[pl.ds(0, m), :], own_ref, own_sem)

    def last_copy(r, j):
        return pltpu.make_async_remote_copy(
            src_ref=send_buf.at[r * subs + j],
            dst_ref=sum_ref.at[rows_of(0, r, j), :],
            send_sem=rs_send.at[r * subs + j],
            recv_sem=last_recv.at[r * subs + j],
            device_id={"tp": target[r]},
            device_id_type=pl.DeviceIdType.MESH,
        )

    def rs_add(p, r, first):
        h, j = p // subs + 1, p % subs
        term_copy(p, r).wait()
        total = term_buf[p % 2, r]
        if not first:
            rs_copy(h - 1, r, j).wait_recv()
            rs_copy(h - 1, r, j).wait_send()
            total += sum_buf[h % HOP_SLOTS * per_hop + r * subs + j].astype(F32)
        send_buf[r * subs + j] = total.astype(BF16)
        if not first:

            @pl.when(h + HOP_SLOTS < n)
            def _():
                pl.semaphore_signal(
                    credit.at[r * subs + j],
                    inc=1,
                    device_id={"tp": origin[r]},
                    device_id_type=pl.DeviceIdType.MESH,
                )

    def rs_service(p, first, last=False):
        h, j = p // subs + 1, p % subs
        for r in range(RINGS):
            rs_add(p, r, first)
        for r in range(RINGS):
            if not first and not last:

                @pl.when(h > HOP_SLOTS)
                def _():
                    pl.semaphore_wait(credit.at[r * subs + j], 1)

            if last:
                last_copy(r, j).start()
            else:
                rs_copy(h, r, j).start()
        if not last:
            term_start(p + 1)
        elif p + 1 < (n - 1) * subs:
            term_start(p + 1)

    def gu_copies(g):
        k = pl.ds(pl.multiple_of(g % K_TILES * kt, kt), kt)
        slot = g % WEIGHT_SLOTS
        return (
            pltpu.make_async_copy(wg_ref.at[k, :], wg_buf.at[slot], wgu_sem.at[slot, 0]),
            pltpu.make_async_copy(wu_ref.at[k, :], wu_buf.at[slot], wgu_sem.at[slot, 1]),
        )

    def wd_copy(e):
        cols = pl.ds(pl.multiple_of(e % N_TILES * nt, nt), nt)
        slot = e % WEIGHT_SLOTS
        return pltpu.make_async_copy(wd_ref.at[:, cols], wd_buf.at[slot], wd_sem.at[slot])

    def x_start(b, i):
        k = pl.ds(pl.multiple_of(i * kt, kt), kt)

        @pl.when(b == 0)
        def _():
            pltpu.make_async_copy(
                x_ref.at[:, k], x_buf.at[i % X_SLOTS, pl.ds(0, m), :], x_sem.at[i % X_SLOTS]
            ).start()
            pltpu.make_async_copy(
                xg_ref.at[pl.ds(m, block - m), k], x_buf.at[i % X_SLOTS, pl.ds(m, block - m), :], x_sem.at[i % X_SLOTS]
            ).start()

        @pl.when(b > 0)
        def _():
            x_copy(b, i).start()

    def x_copy(b, i):
        k = pl.ds(pl.multiple_of(i * kt, kt), kt)
        return pltpu.make_async_copy(
            xg_ref.at[pl.ds(pl.multiple_of(b * block, block), block), k], x_buf.at[i % X_SLOTS], x_sem.at[i % X_SLOTS]
        )

    def t_copy(b, i):
        rows = pl.ds(pl.multiple_of(b * block, block), block)
        cols = pl.ds(pl.multiple_of(i * nt, nt), nt)
        return pltpu.make_async_copy(t_buf.at[i % 2], t_ref.at[rows, cols], t_sem.at[i % 2])

    def t_drain(b):
        t_copy(b, N_TILES - 2).wait()
        t_copy(b, N_TILES - 1).wait()

    f = wg_ref.shape[1]
    step_n = 256

    def gate_up(b, i):
        g = b * K_TILES + i
        slot = g % WEIGHT_SLOTS

        @pl.when(i == 0)
        def _():
            @pl.when(b > 0)
            def _():
                t_drain(b - 1)

            acc_g[...] = jnp.zeros_like(acc_g)
            acc_u[...] = jnp.zeros_like(acc_u)

        @pl.when(i + X_SLOTS - 1 < K_TILES)
        def _():
            x_start(b, i + X_SLOTS - 1)

        @pl.when(g + WEIGHT_SLOTS - 1 < BLOCKS * K_TILES)
        def _():
            for copy in gu_copies(g + WEIGHT_SLOTS - 1):
                copy.start()

        x_copy(b, i).wait()
        for copy in gu_copies(g):
            copy.wait()

        if COMPUTE:
            xt = x_buf[i % X_SLOTS]
            for c in range(0, f, step_n):
                acc_g[:, c : c + step_n] += jnp.dot(xt, wg_buf[slot, :, c : c + step_n], preferred_element_type=F32)
                acc_u[:, c : c + step_n] += jnp.dot(xt, wu_buf[slot, :, c : c + step_n], preferred_element_type=F32)

        @pl.when(i == K_TILES - 1)
        def _():
            def chunk(c, _):
                rows = pl.ds(pl.multiple_of(c * 16, 16), 16)
                hid[rows, :] = (jax.nn.silu(acc_g[rows, :]) * acc_u[rows, :]).astype(BF16)
                return 0

            lax.fori_loop(0, block // 16, chunk, 0)

    def down(b, i):
        e = b * N_TILES + i
        slot = e % WEIGHT_SLOTS
        wd_copy(e).wait()

        @pl.when(e + WEIGHT_SLOTS - 1 < BLOCKS * N_TILES)
        def _():
            wd_copy(e + WEIGHT_SLOTS - 1).start()

        @pl.when(i >= 2)
        def _():
            t_copy(b, i - 2).wait()

        if COMPUTE:
            for c in range(0, nt, step_n):
                t_buf[i % 2, :, c : c + step_n] = jnp.dot(
                    hid[...], wd_buf[slot, :, c : c + step_n], preferred_element_type=F32
                )
        t_copy(b, i).start()

        ahead = i - (N_TILES - X_SLOTS + 1)

        @pl.when((ahead >= 0) & (b < BLOCKS - 1))
        def _():
            x_start(b + 1, ahead)

    barrier = pltpu.get_barrier_semaphore()
    for r in range(RINGS):
        pl.semaphore_signal(barrier, inc=1, device_id={"tp": target[r]}, device_id_type=pl.DeviceIdType.MESH)
    pl.semaphore_wait(barrier, RINGS)

    if COMM:
        ag_first()
    for e in range(WEIGHT_SLOTS - 1):
        for copy in gu_copies(e):
            copy.start()
        wd_copy(e).start()

    ticks = K_TILES + N_TILES
    total = BLOCKS * ticks
    lead = (n // BLOCKS - 1) * subs
    forwards = (n - 2) * subs
    last_terms = (n - n // BLOCKS - 1) * subs

    def serve(z):
        @pl.when(z < forwards)
        def _():
            ag_service(z)

        @pl.when(z == forwards - 1)
        def _():
            term_start(0)
            own_copy().start()

        @pl.when((z >= forwards) & (z < forwards + subs))
        def _():
            rs_service(z - forwards, True)

        @pl.when(z >= forwards + subs)
        def _():
            rs_service(z - forwards, False)

        @pl.when((z >= forwards + subs) & (z < forwards + 2 * subs))
        def _():
            ag_last(z - forwards - subs)

    if COMM:
        lax.fori_loop(0, lead, lambda q, _: (ag_service(q), 0)[1], 0)
    for i in range(X_SLOTS - 1):
        x_start(0, i)

    def tick(t, _):
        b, i = t // ticks, t % ticks

        @pl.when(i < K_TILES)
        def _():
            gate_up(b, i)

        @pl.when(i >= K_TILES)
        def _():
            down(b, i - K_TILES)

        if COMM:
            u = t * (forwards - lead)

            @pl.when((t < GATHER_TICKS) & (u % GATHER_TICKS < forwards - lead))
            def _():
                serve(lead + u // GATHER_TICKS)

            v = (t - GATHER_TICKS) * (last_terms - 1)
            rest = total - GATHER_TICKS

            @pl.when((t >= GATHER_TICKS) & (v % rest < last_terms - 1))
            def _():
                serve(forwards + v // rest)

        return 0

    lax.fori_loop(0, total, tick, 0)
    t_drain(BLOCKS - 1)
    if COMM:
        lax.fori_loop(last_terms - 1, (n - 2) * subs, lambda p, _: (rs_service(p, False), 0)[1], 0)
        for j in range(subs):
            rs_service((n - 2) * subs + j, False, True)
        for j in range(subs):
            for r in range(RINGS):
                last_copy(r, j).wait_recv()
                last_copy(r, j).wait_send()
        own_copy().wait()


def solution(mesh):
    n = mesh.shape["tp"]

    def step(x, w_gate, w_up, w_down):
        m, d = x.shape
        f = w_gate.shape[1]
        block = n * m // BLOCKS
        kt, nt = d // K_TILES, d // N_TILES
        subs = m // RINGS // ROWS
        per_hop = RINGS * subs
        dma = pltpu.SemaphoreType.DMA
        hbm = pl.BlockSpec(memory_space=pl.ANY)
        sums, own, _, _ = pl.pallas_call(
            functools.partial(kernel, n),
            out_shape=(
                jax.ShapeDtypeStruct((m, d), BF16),
                jax.ShapeDtypeStruct((m, d), F32),
                jax.ShapeDtypeStruct((n * m, d), BF16),
                jax.ShapeDtypeStruct((n * m, d), F32),
            ),
            in_specs=[hbm] * 4,
            out_specs=(hbm,) * 4,
            scratch_shapes=[
                pltpu.VMEM((WEIGHT_SLOTS, kt, f), BF16),
                pltpu.VMEM((WEIGHT_SLOTS, kt, f), BF16),
                pltpu.VMEM((WEIGHT_SLOTS, f, nt), BF16),
                pltpu.VMEM((X_SLOTS, block, kt), BF16),
                pltpu.VMEM((block, f), F32),
                pltpu.VMEM((block, f), F32),
                pltpu.VMEM((block, f), BF16),
                pltpu.VMEM((2, block, nt), F32),
                pltpu.VMEM((2, RINGS, ROWS, d), F32),
                pltpu.VMEM((per_hop, ROWS, d), BF16),
                pltpu.VMEM((HOP_SLOTS * per_hop, ROWS, d), BF16),
                dma((WEIGHT_SLOTS, 2)),
                dma((WEIGHT_SLOTS,)),
                dma((X_SLOTS,)),
                dma((2,)),
                dma((2, RINGS)),
                dma(()),
                dma((per_hop,)),
                dma(((n - 1) * per_hop,)),
                dma((per_hop,)),
                dma((HOP_SLOTS * per_hop,)),
                dma((per_hop,)),
                pltpu.SemaphoreType.REGULAR((per_hop,)),
            ],
            compiler_params=pltpu.CompilerParams(
                collective_id=0, has_side_effects=True, vmem_limit_bytes=47_000_000
            ),
        )(pltpu.with_memory_space_constraint(x, pltpu.HBM), w_gate, w_up, w_down)
        return (sums.astype(F32) + own).astype(BF16)

    return jax.shard_map(
        step,
        mesh=mesh,
        in_specs=(P(("dp", "tp"), None), P(None, "tp"), P(None, "tp"), P("tp", None)),
        out_specs=P(("dp", "tp"), None),
        check_vma=False,
    )
```
